32 devices in a mesh: ta: 4 (over y, x), gx: 8 (over z, core).
Axes of the slice: x: 2, y: 2, z: 4, core: 2. Of those that a mesh axis runs over, the one named last changes fastest.
Arguments:
- eigvecs: bfloat16 [4, 4096, 3, 2, 384], P('ta', 'gx'), may hold values from -0.0390625 to 0.0390625
- perambulators: bfloat16 [4, 2, 384, 4, 4, 384], P('ta', None, 'gx'), may hold values from -0.59765625 to 0.59765625
- source_blocks: bfloat16 [9, 2, 384, 384], replicated, may hold values from -0.3125 to 0.3125
- momenta: int32 [9, 3], replicated, may hold values from -2 to 2
- op_momentum: int32 [64], replicated, may hold values from 0 to 8
- op_gamma: int32 [64], replicated, may hold values from 0 to 15
- ref_vectors: float32 [2, 64, 8], replicated, may hold values from -0.75 to 0.75
Outputs:
- correlator: float32 [4, 2, 64, 64], P('ta')
- projected: float32 [4, 2, 8, 8], P('ta')
The draws below stay inside these ranges and needn't reach their ends.
All inputs are finite; a program needn't handle non-finite values.
Results may differ from the reference program's by a relative error of at most 0.0055.
Values may be sent and summed in bfloat16 or wider, within the bound.
A program may use at most 128 MiB of HBM per device.

```python
import math
import jax
import jax.numpy as jnp
import numpy as np
from jax import lax

EXTENT = 96
NEV = 384
NMOM = 9
NOPS = 64
NVEC = 8
TIMES = 4
SPACE = 4096


def set_ends(result, key, least, largest):
    spot = [jax.random.randint(jax.random.fold_in(key, axis), (), 0, length) for axis, length in enumerate(result.shape)]
    widest = result.shape.index(max(result.shape))
    neighbour = spot[:widest] + [(spot[widest] + 1) % result.shape[widest]] + spot[widest + 1:]
    return result.at[tuple(spot)].set(least).at[tuple(neighbour)].set(largest)


def levels(stream_key, extent, split, smallest, top_value):
    level = 1.0
    for dim, parts in split:
        steps = jax.random.uniform(jax.random.fold_in(jax.random.fold_in(stream_key, 6), dim), (parts,), jnp.float32, smallest / len(split), top_value / len(split))
        level = level * jnp.repeat(jnp.exp(steps), extent[dim] // parts).reshape((-1,) + (1,) * (len(extent) - 1 - dim))
    return level


def bell_draw(key, extent, width, reach, split=(), held_as=jnp.bfloat16):
    entries = width * jax.random.normal(key, extent, jnp.float32)
    if split:
        entries = entries * levels(key, extent, split, -0.22, 0.18)
    return jnp.clip(entries, -reach, reach).astype(held_as)


def setup_inputs(seed: int = 0) -> dict:
    arg_keys = jax.random.split(jax.random.key(seed), 8)
    eigvecs = bell_draw(arg_keys[0], (TIMES, SPACE, 3, 2, NEV), (6 * SPACE) ** -0.5, 0.0390625, ((0, 4), (1, 8)))
    perambulators = bell_draw(arg_keys[1], (TIMES, 2, NEV, 4, 4, NEV), 0.1, 0.59765625, ((0, 4), (2, 8)))
    source_blocks = bell_draw(arg_keys[2], (NMOM, 2, NEV, NEV), NEV ** -0.5, 0.3125)
    momenta = set_ends(jax.random.randint(arg_keys[3], (NMOM, 3), -2, 3), jax.random.fold_in(arg_keys[3], 1), -2, 2).astype(jnp.int32)
    op_momentum = set_ends(jax.random.randint(arg_keys[4], (NOPS,), 0, NMOM), jax.random.fold_in(arg_keys[4], 1), 0, NMOM - 1).astype(jnp.int32)
    op_gamma = set_ends(jax.random.randint(arg_keys[5], (NOPS,), 0, 16), jax.random.fold_in(arg_keys[5], 1), 0, 15).astype(jnp.int32)
    ref_vectors = bell_draw(arg_keys[6], (2, NOPS, NVEC), NOPS ** -0.5, 0.75, (), jnp.float32)
    return dict(eigvecs=eigvecs, perambulators=perambulators, source_blocks=source_blocks, momenta=momenta, op_momentum=op_momentum, op_gamma=op_gamma, ref_vectors=ref_vectors)


full_precision = lax.Precision.HIGHEST

def gamma_tables():
    zero_block = np.zeros((4, 4), np.float32)
    first_imag = np.array([[0, 0, 0, 1], [0, 0, 1, 0], [0, -1, 0, 0], [-1, 0, 0, 0]], np.float32)
    second_real = np.array([[0, 0, 0, -1], [0, 0, 1, 0], [0, 1, 0, 0], [-1, 0, 0, 0]], np.float32)
    third_imag = np.array([[0, 0, 1, 0], [0, 0, 0, -1], [-1, 0, 0, 0], [0, 1, 0, 0]], np.float32)
    fourth_real = np.array([[0, 0, 1, 0], [0, 0, 0, 1], [1, 0, 0, 0], [0, 1, 0, 0]], np.float32)
    gamma_list = [(zero_block, first_imag), (second_real, zero_block), (zero_block, third_imag), (fourth_real, zero_block)]
    real_parts = []
    imag_parts = []
    for subset in range(16):
        prod_real = np.eye(4, dtype=np.float32)
        prod_imag = np.zeros((4, 4), np.float32)
        for position in range(4):
            if subset >> position & 1:
                factor_real, factor_imag = gamma_list[position]
                prod_real, prod_imag = (prod_real @ factor_real - prod_imag @ factor_imag, prod_real @ factor_imag + prod_imag @ factor_real)
        real_parts.append(prod_real)
        imag_parts.append(prod_imag)
    return (np.stack(real_parts).astype(np.float32), np.stack(imag_parts).astype(np.float32))

def complex_einsum(form, left_real, left_imag, right_real, right_imag):

    def single(left_part, right_part):
        return jnp.einsum(form, left_part, right_part, precision=full_precision, preferred_element_type=jnp.float32)
    return (single(left_real, right_real) - single(left_imag, right_imag), single(left_real, right_imag) + single(left_imag, right_real))

def phase_factors(momenta, site_ids):
    xcoord = site_ids % EXTENT
    ycoord = site_ids // EXTENT % EXTENT
    zcoord = site_ids // (EXTENT * EXTENT)
    winding = (momenta[:, 0:1] * xcoord[None, :] + momenta[:, 1:2] * ycoord[None, :] + momenta[:, 2:3] * zcoord[None, :]) % EXTENT
    phase_angle = winding.astype(jnp.float32) * (-2.0 * math.pi / EXTENT)
    return (jnp.cos(phase_angle), jnp.sin(phase_angle))

def right_block(vec_real, vec_imag, cosine, sine_row):
    cosine = cosine[:, None, None]
    sine_row = sine_row[:, None, None]
    eig_width = vec_real.shape[-1]
    twist_real = (cosine * vec_real - sine_row * vec_imag).astype(jnp.bfloat16).reshape(-1, eig_width)
    twist_imag = (cosine * vec_imag + sine_row * vec_real).astype(jnp.bfloat16).reshape(-1, eig_width)
    upper = jnp.concatenate([twist_real, twist_imag], 1)
    lower = jnp.concatenate([twist_imag, -twist_real], 1)
    return jnp.concatenate([upper, lower], 0)

def assemble(blocks_real, blocks_imag, op_momentum, op_gamma):
    table_real, table_imag = gamma_tables()
    chosen = (op_gamma[:, None] == jnp.arange(16, dtype=jnp.int32)[None, :]).astype(jnp.float32)
    gre = jnp.einsum('ig,gax->iax', chosen, jnp.asarray(table_real), precision=full_precision)
    gim = jnp.einsum('ig,gax->iax', chosen, jnp.asarray(table_imag), precision=full_precision)
    moment = (op_momentum[:, None] == jnp.arange(NMOM, dtype=jnp.int32)[None, :]).astype(jnp.float32)
    chiral = jnp.asarray(np.array([1.0, 1.0, -1.0, -1.0], np.float32))
    weight_left = moment[:, :, None, None] * chiral[None, None, None, :]
    left_real = weight_left * jnp.transpose(gre, (0, 2, 1))[:, None]
    left_imag = weight_left * jnp.transpose(gim, (0, 2, 1))[:, None]
    lifted_real, lifted_imag = complex_einsum('imxa,mxynwa->iynw', left_real, left_imag, blocks_real, blocks_imag)
    weight_right = moment[:, :, None, None] * chiral[None, None, None, :]
    right_real = weight_right * jnp.transpose(gre, (0, 2, 1))[:, None]
    right_imag = -weight_right * jnp.transpose(gim, (0, 2, 1))[:, None]
    return complex_einsum('iynw,jnyw->ij', lifted_real, lifted_imag, right_real, right_imag)

def project(corr_real, corr_imag, ref_vectors):
    basis_real = ref_vectors[0]
    basis_imag = ref_vectors[1]
    half_real, half_imag = complex_einsum('ij,jv->iv', corr_real, corr_imag, basis_real, basis_imag)
    return complex_einsum('iu,iv->uv', basis_real, -basis_imag, half_real, half_imag)

def reference(eigvecs, perambulators, source_blocks, momenta, op_momentum, op_gamma, ref_vectors):
    site_ids = jnp.arange(SPACE, dtype=jnp.int32)
    cosine, sine_row = phase_factors(momenta, site_ids)
    correlators = []
    raw_list = []
    for slice_index in range(TIMES):
        vectors = eigvecs[slice_index]
        vec_real = vectors[:, :, 0, :]
        vec_imag = vectors[:, :, 1, :]
        conj_left = jnp.concatenate([vec_real.reshape(-1, NEV), vec_imag.reshape(-1, NEV)], 0).astype(jnp.float32)
        pieces = []
        for moment_index in range(NMOM):
            twist_right = right_block(vec_real, vec_imag, cosine[moment_index], sine_row[moment_index]).astype(jnp.float32)
            summed = lax.dot_general(conj_left, twist_right, (((0,), (0,)), ((), ())), precision=full_precision, preferred_element_type=jnp.float32)
            pieces.append(summed.reshape(NEV, 2, NEV))
        phase_rows = jnp.stack(pieces, 1).astype(jnp.bfloat16).astype(jnp.float32)
        peram = perambulators[slice_index].astype(jnp.float32)
        sink_real, sink_imag = complex_einsum('rml,labk->mrabk', phase_rows[:, :, 0], phase_rows[:, :, 1], peram[0], peram[1])
        sink_real = sink_real.astype(jnp.bfloat16).astype(jnp.float32)
        sink_imag = sink_imag.astype(jnp.bfloat16).astype(jnp.float32)
        source = source_blocks.astype(jnp.float32)
        src_real, src_imag = complex_einsum('rabl,nkl->rabnk', peram[0], -peram[1], source[:, 0], source[:, 1])
        src_real = src_real.astype(jnp.bfloat16).astype(jnp.float32)
        src_imag = src_imag.astype(jnp.bfloat16).astype(jnp.float32)
        blocks_real, blocks_imag = complex_einsum('mrxyk,rawnk->mxynwa', sink_real, sink_imag, src_real, src_imag)
        corr_real, corr_imag = assemble(blocks_real, blocks_imag, op_momentum, op_gamma)
        correlators.append(jnp.stack([corr_real, corr_imag]))
        proj_real, proj_imag = project(corr_real, corr_imag, ref_vectors)
        raw_list.append(jnp.stack([proj_real, proj_imag]))
    first = raw_list[0]
    mean_square = jnp.mean(first * first)
    scale_factor = lax.rsqrt(mean_square + 1e-06)
    return (jnp.stack(correlators), jnp.stack(raw_list) * scale_factor)
```

```python
import functools
import math

import jax
import jax.numpy as jnp
import numpy as np
from jax import lax
from jax.experimental import pallas as pl
from jax.experimental.pallas import tpu as pltpu
from jax.sharding import PartitionSpec as P

EXTENT = 96
NMOM = 9


full_precision = lax.Precision.HIGHEST


def gamma_tables():
    zero_block = np.zeros((4, 4), np.float32)
    first_imag = np.array([[0, 0, 0, 1], [0, 0, 1, 0], [0, -1, 0, 0], [-1, 0, 0, 0]], np.float32)
    second_real = np.array([[0, 0, 0, -1], [0, 0, 1, 0], [0, 1, 0, 0], [-1, 0, 0, 0]], np.float32)
    third_imag = np.array([[0, 0, 1, 0], [0, 0, 0, -1], [-1, 0, 0, 0], [0, 1, 0, 0]], np.float32)
    fourth_real = np.array([[0, 0, 1, 0], [0, 0, 0, 1], [1, 0, 0, 0], [0, 1, 0, 0]], np.float32)
    gamma_list = [
        (zero_block, first_imag),
        (second_real, zero_block),
        (zero_block, third_imag),
        (fourth_real, zero_block),
    ]
    real_parts = []
    imag_parts = []
    for subset in range(16):
        prod_real = np.eye(4, dtype=np.float32)
        prod_imag = np.zeros((4, 4), np.float32)
        for position in range(4):
            if subset >> position & 1:
                factor_real, factor_imag = gamma_list[position]
                prod_real, prod_imag = (
                    prod_real @ factor_real - prod_imag @ factor_imag,
                    prod_real @ factor_imag + prod_imag @ factor_real,
                )
        real_parts.append(prod_real)
        imag_parts.append(prod_imag)
    return (np.stack(real_parts).astype(np.float32), np.stack(imag_parts).astype(np.float32))


def phase_factors(momenta, site_ids):
    xcoord = site_ids % EXTENT
    ycoord = site_ids // EXTENT % EXTENT
    zcoord = site_ids // (EXTENT * EXTENT)
    winding = (
        momenta[:, 0:1] * xcoord[None, :]
        + momenta[:, 1:2] * ycoord[None, :]
        + momenta[:, 2:3] * zcoord[None, :]
    ) % EXTENT
    phase_angle = winding.astype(jnp.float32) * (-2.0 * math.pi / EXTENT)
    return (jnp.cos(phase_angle), jnp.sin(phase_angle))


PAD = 24
MESH = pl.DeviceIdType.MESH


def nn_dot(left, right, precision=None):
    return lax.dot_general(
        left, right, (((1,), (0,)), ((), ())), precision=precision, preferred_element_type=jnp.float32
    )


def nt_dot(left, right):
    return lax.dot_general(
        left, right, (((1,), (1,)), ((), ())), preferred_element_type=jnp.float32
    )


def turn_kernel(fields_ref, turned_ref):
    turned_ref[...] = fields_ref[...].astype(jnp.float32).T.astype(jnp.bfloat16)


def turn_fields(fields):
    sites, wide = fields.shape
    width = wide // 6
    return pl.pallas_call(
        turn_kernel,
        grid=(6,),
        out_shape=jax.ShapeDtypeStruct((width, 6 * sites), jnp.bfloat16),
        in_specs=[pl.BlockSpec((sites, width), lambda i: (0, i))],
        out_specs=pl.BlockSpec((width, sites), lambda i: (0, i)),
        cost_estimate=pl.CostEstimate(flops=10**9, bytes_accessed=4 * sites * wide, transcendentals=0),
    )(fields)


def phase_kernel(fields_ref, turned_ref, cos_ref, sin_ref, out_ref):
    sites, wide = fields_ref.shape
    width = wide // 6
    cosine = cos_ref[0]
    sine_row = sin_ref[0]
    total = None
    for colour in range(3):
        start = 2 * colour * width
        vec_real = fields_ref[:, start : start + width].astype(jnp.float32)
        vec_imag = fields_ref[:, start + width : start + 2 * width].astype(jnp.float32)
        twist_real = (cosine * vec_real - sine_row * vec_imag).astype(jnp.bfloat16)
        twist_imag = (cosine * vec_imag + sine_row * vec_real).astype(jnp.bfloat16)
        upper = jnp.concatenate([twist_real, twist_imag], 1)
        lower = jnp.concatenate([twist_imag, -twist_real], 1)
        right = jnp.concatenate([upper, lower], 0)
        part = nn_dot(turned_ref[:, 2 * colour * sites : 2 * (colour + 1) * sites], right)
        total = part if total is None else total + part
    out_ref[0] = total


def phase_partials(fields, turned, cosine, sine_row):
    sites, wide = fields.shape
    width = wide // 6
    count = cosine.shape[0]
    return pl.pallas_call(
        phase_kernel,
        grid=(count,),
        out_shape=jax.ShapeDtypeStruct((count, width, 2 * width), jnp.float32),
        in_specs=[
            pl.BlockSpec((sites, wide), lambda m: (0, 0)),
            pl.BlockSpec((width, 6 * sites), lambda m: (0, 0)),
            pl.BlockSpec((1, sites, 1), lambda m: (m, 0, 0)),
            pl.BlockSpec((1, sites, 1), lambda m: (m, 0, 0)),
        ],
        out_specs=pl.BlockSpec((1, width, 2 * width), lambda m: (m, 0, 0)),
        cost_estimate=pl.CostEstimate(
            flops=24 * count * sites * width * width,
            bytes_accessed=8 * count * width * width,
            transcendentals=0,
        ),
    )(fields, turned, cosine[:, :, None], sine_row[:, :, None])


def source_kernel(rows_ref, block_ref, out_ref):
    shape = out_ref.shape[2:]
    width = out_ref.shape[-1]
    rows = jnp.concatenate([rows_ref[0], rows_ref[1]], 1)
    real = block_ref[0, 0]
    imag = block_ref[0, 1]
    weights = jnp.concatenate(
        [jnp.concatenate([real, imag], 1), jnp.concatenate([imag, -real], 1)], 0
    )
    product = nt_dot(rows, weights).astype(jnp.bfloat16)
    out_ref[0, 0] = product[:, :width].reshape(shape)
    out_ref[1, 0] = product[:, width:].reshape(shape)


def source_products(rows, source_blocks):
    _, high, width = rows.shape
    count = source_blocks.shape[0]
    return pl.pallas_call(
        source_kernel,
        grid=(count,),
        out_shape=jax.ShapeDtypeStruct((2, count, high // 16, 16, width), jnp.bfloat16),
        in_specs=[
            pl.BlockSpec((2, high, width), lambda n: (0, 0, 0)),
            pl.BlockSpec((1, 2, width, width), lambda n: (n, 0, 0, 0)),
        ],
        out_specs=pl.BlockSpec((2, 1, high // 16, 16, width), lambda n: (0, n, 0, 0, 0)),
        cost_estimate=pl.CostEstimate(
            flops=8 * count * high * width * width,
            bytes_accessed=4 * count * high * width,
            transcendentals=0,
        ),
    )(rows, source_blocks)


def sink_kernel(left_ref, right_ref, out_ref):
    width = right_ref.shape[-1]
    shape = out_ref.shape[1:]
    right = jnp.concatenate(
        [
            jnp.concatenate(
                [right_ref[:, spin, part].reshape(-1, width) for part in range(2)], 0
            )
            for spin in range(2)
        ],
        1,
    )
    product = nn_dot(left_ref[...], right).astype(jnp.bfloat16)
    out_ref[0] = product[:, :width].reshape(shape)
    out_ref[1] = product[:, width:].reshape(shape)


def sink_products(left, right):
    high = left.shape[0]
    owners, spins, _, depth, width = right.shape
    return pl.pallas_call(
        sink_kernel,
        grid=(spins // 2,),
        out_shape=jax.ShapeDtypeStruct((spins, high // PAD, PAD, width), jnp.bfloat16),
        in_specs=[
            pl.BlockSpec((high, 2 * width), lambda x: (0, 0)),
            pl.BlockSpec((owners, 2, 2, depth, width), lambda x: (0, x, 0, 0, 0)),
        ],
        out_specs=pl.BlockSpec((2, high // PAD, PAD, width), lambda x: (x, 0, 0, 0)),
        cost_estimate=pl.CostEstimate(
            flops=4 * spins * high * width * width,
            bytes_accessed=4 * spins * high * width,
            transcendentals=0,
        ),
    )(left, right)


def three_parts(value):
    parts = []
    for _ in range(3):
        part = value.astype(jnp.bfloat16)
        parts.append(part)
        value = value - part.astype(jnp.float32)
    return parts


def correlate_kernel(sink_ref, src_ref, left_ref, right_ref, out_ref, total_ref):
    step = pl.program_id(0)
    width = sink_ref.shape[-1]
    picks = sink_ref.shape[1]
    product = None
    for start in range(0, picks, 2):
        pair = range(start, start + 2)
        first = jnp.concatenate([src_ref[:, index].reshape(-1, width) for index in pair], 1)
        second = jnp.concatenate([sink_ref[:, index].reshape(-1, width) for index in pair], 1)
        part = nt_dot(first, second)
        product = part if product is None else product + part

    @pl.when(step == 0)
    def _():
        total_ref[...] = product

    @pl.when(step > 0)
    def _():
        total_ref[...] += product

    @pl.when(step == pl.num_programs(0) - 1)
    def _():
        high, wide = total_ref.shape
        ops = left_ref.shape[1] // 4
        span = wide // 4
        row_spin = lax.broadcasted_iota(jnp.int32, (high, 1), 0) // 4 % 4
        answer = jnp.zeros((ops, ops), jnp.float32)
        for spin in range(4):
            spread = jnp.zeros((high, 4 * ops), jnp.float32)
            for part in three_parts(total_ref[:, spin * span : (spin + 1) * span]):
                spread = spread + nn_dot(part, left_ref[...])
            lifted = spread[:, :ops]
            for other in range(1, 4):
                lifted = jnp.where(
                    row_spin == other, spread[:, other * ops : (other + 1) * ops], lifted
                )
            for part in three_parts(lifted):
                answer = answer + nn_dot(right_ref[spin], part)
        half = ops // 2
        answer = answer.T
        real = answer[:half] - pltpu.roll(answer[half:], half, 1)
        imag = pltpu.roll(answer[:half], half, 1) + answer[half:]
        lane = lax.broadcasted_iota(jnp.int32, real.shape, 1)
        out_ref[...] = jnp.where(lane < half, real, pltpu.roll(imag, half, 1))


def correlate(sink, src, left, right):
    spins, rows, pad, width = sink.shape
    count = src.shape[0]
    picks = 4
    ops = left.shape[1] // 4
    return pl.pallas_call(
        correlate_kernel,
        grid=(rows // picks,),
        out_shape=jax.ShapeDtypeStruct((ops // 2, ops), jnp.float32),
        in_specs=[
            pl.BlockSpec((spins, picks, pad, width), lambda r: (0, r, 0, 0)),
            pl.BlockSpec((count, picks, spins, width), lambda r: (0, r, 0, 0)),
            pl.BlockSpec(left.shape, lambda r: (0, 0)),
            pl.BlockSpec(right.shape, lambda r: (0, 0, 0)),
        ],
        out_specs=pl.BlockSpec((ops // 2, ops), lambda r: (0, 0)),
        scratch_shapes=[pltpu.VMEM((count * spins, spins * pad), jnp.float32)],
        cost_estimate=pl.CostEstimate(
            flops=2 * rows * spins * pad * count * spins * width,
            bytes_accessed=2 * rows * spins * width * (pad + count),
            transcendentals=0,
        ),
    )(sink, src, left, right)


def finish_kernel(
    groups, slices, part_ref, basis_ref, turned_ref, corr_ref, proj_ref,
    slots, squares, send_sem, recv_sem, square_send, square_recv,
):
    me = lax.axis_index("gx")
    here = lax.axis_index("ta")
    barrier = pltpu.get_barrier_semaphore()
    for step in range(1, groups):
        peer = lax.rem(me + step, groups)
        pl.semaphore_signal(barrier, inc=1, device_id={"gx": peer}, device_id_type=MESH)
    for step in range(1, slices):
        peer = lax.rem(here + step, slices)
        pl.semaphore_signal(barrier, inc=1, device_id={"ta": peer}, device_id_type=MESH)
    pl.semaphore_wait(barrier, groups + slices - 2)
    copies = []
    for step in range(1, groups):
        copies.append(
            pltpu.make_async_remote_copy(
                src_ref=part_ref,
                dst_ref=slots.at[me],
                send_sem=send_sem.at[step],
                recv_sem=recv_sem.at[step],
                device_id={"gx": lax.rem(me + step, groups)},
                device_id_type=MESH,
            )
        )
    for copy in copies:
        copy.start()
    slots[me] = part_ref[...]
    for copy in copies:
        copy.wait()
    total = slots[0]
    for index in range(1, groups):
        total = total + slots[index]
    half = total.shape[0]
    real = total[:, :half]
    imag = total[:, half:]
    corr_ref[0] = real
    corr_ref[1] = imag

    def product(left, right):
        return nn_dot(left, right, full_precision)

    mid_real = product(real, basis_ref[0]) - product(imag, basis_ref[1])
    mid_imag = product(real, basis_ref[1]) + product(imag, basis_ref[0])
    raw_real = product(turned_ref[0], mid_real) + product(turned_ref[1], mid_imag)
    raw_imag = product(turned_ref[0], mid_imag) - product(turned_ref[1], mid_real)
    vectors = raw_real.shape[0]
    square = jnp.sum(
        jnp.sum(raw_real * raw_real + raw_imag * raw_imag, 1, keepdims=True), 0, keepdims=True
    ) / (2 * vectors * vectors)
    squares[here] = jnp.broadcast_to(square, squares.shape[1:])
    copies = []
    for step in range(1, slices):
        copies.append(
            pltpu.make_async_remote_copy(
                src_ref=squares.at[here],
                dst_ref=squares.at[here],
                send_sem=square_send.at[step],
                recv_sem=square_recv.at[step],
                device_id={"ta": lax.rem(here + step, slices)},
                device_id_type=MESH,
            )
        )
    for copy in copies:
        copy.start()
    for copy in copies:
        copy.wait()
    scale = lax.rsqrt(squares[0] + 1e-06)[:vectors]
    proj_ref[0] = (raw_real * scale)[:, :vectors]
    proj_ref[1] = (raw_imag * scale)[:, :vectors]


def finish(part, ref_vectors):
    groups = lax.axis_size("gx")
    slices = lax.axis_size("ta")
    half, wide = part.shape
    vectors = ref_vectors.shape[-1]
    basis = jnp.pad(ref_vectors, ((0, 0), (0, 0), (0, 128 - vectors)))
    turned = jnp.transpose(ref_vectors, (0, 2, 1))
    vmem = pl.BlockSpec(memory_space=pltpu.VMEM)
    return pl.pallas_call(
        functools.partial(finish_kernel, groups, slices),
        out_shape=(
            jax.ShapeDtypeStruct((2, half, half), jnp.float32),
            jax.ShapeDtypeStruct((2, vectors, vectors), jnp.float32),
        ),
        in_specs=[vmem, vmem, vmem],
        out_specs=(vmem, vmem),
        scratch_shapes=[
            pltpu.VMEM((groups, half, wide), jnp.float32),
            pltpu.VMEM((slices, 8, 128), jnp.float32),
            pltpu.SemaphoreType.DMA((groups,)),
            pltpu.SemaphoreType.DMA((groups,)),
            pltpu.SemaphoreType.DMA((slices,)),
            pltpu.SemaphoreType.DMA((slices,)),
        ],
        compiler_params=pltpu.CompilerParams(collective_id=0, has_side_effects=True),
    )(part, basis, turned)


def spin_weights(op_momentum, op_gamma):
    table_real, table_imag = gamma_tables()
    chosen = (op_gamma[:, None] == jnp.arange(16, dtype=jnp.int32)[None, :]).astype(jnp.float32)
    gre = jnp.einsum("ig,gax->iax", chosen, jnp.asarray(table_real), precision=full_precision)
    gim = jnp.einsum("ig,gax->iax", chosen, jnp.asarray(table_imag), precision=full_precision)
    moment = (op_momentum[:, None] == jnp.arange(NMOM, dtype=jnp.int32)[None, :]).astype(
        jnp.float32
    )
    chiral = jnp.asarray(np.array([1.0, 1.0, -1.0, -1.0], np.float32))
    ops = op_gamma.shape[0]
    gre = gre * chiral[None, :, None]
    gim = gim * chiral[None, :, None]
    left = jnp.stack([jnp.stack([gre, gim], 0), jnp.stack([-gim, gre], 0)], 0)
    left = jnp.transpose(left, (4, 0, 3, 1, 2))[:, :, None] * jnp.transpose(moment)[
        None, None, :, None, None, :
    ]
    left = left.reshape(4, 2 * NMOM, 8 * ops)
    left = jnp.pad(left, ((0, 0), (0, PAD - 2 * NMOM), (0, 0))).reshape(4 * PAD, 8 * ops)
    right = jnp.stack([jnp.stack([gre, -gim], 0), jnp.stack([gim, gre], 0)], 0)
    right = jnp.transpose(right, (4, 1, 2, 0, 3))[:, :, :, :, None, None, :] * moment[
        None, None, :, None, :, None, None
    ]
    right = jnp.broadcast_to(right, (4, 2, ops, 2, NMOM, 4, 4)).reshape(4, 2 * ops, 32 * NMOM)
    return left.astype(jnp.bfloat16), right.astype(jnp.bfloat16)


def combine_rows(partial, row_count):
    size = lax.axis_size("gx")
    chips = size // 2
    me = lax.axis_index("gx")
    core = me % 2
    chip = me // 2
    count, _, width = partial.shape
    split = partial.reshape(count, chips, 2, row_count, width)
    keep = lax.dynamic_index_in_dim(split, core, 2, keepdims=False)
    give = lax.dynamic_index_in_dim(split, 1 - core, 2, keepdims=False).astype(jnp.bfloat16)
    got = lax.ppermute(give, "gx", [(i, i ^ 1) for i in range(size)])
    pair = keep + got.astype(jnp.float32)
    total = lax.dynamic_index_in_dim(pair, chip, 1, keepdims=False)
    for way in (1, -1):
        moved = None
        for step in range(1, chips):
            spot = jnp.clip(chip + way * (chips - step), 0, chips - 1)
            block = lax.dynamic_index_in_dim(pair, spot, 1, keepdims=False)
            if moved is not None:
                block = block + moved.astype(jnp.float32)
            places = [i if way > 0 else chips - 1 - i for i in range(step)]
            links = [(2 * i + c, 2 * (i + way) + c) for i in places for c in range(2)]
            moved = lax.ppermute(block.astype(jnp.bfloat16), "gx", links)
        if moved is not None:
            total = total + moved.astype(jnp.float32)
    return total


def body(eigvecs, perambulators, source_blocks, momenta, op_momentum, op_gamma, ref_vectors):
    vectors = eigvecs[0]
    sites_here = vectors.shape[0]
    eig_width = vectors.shape[-1]
    size = lax.axis_size("gx")
    row_count = eig_width // size
    local = perambulators[0].reshape(2, row_count, 16, eig_width)
    turned_spins = jnp.transpose(perambulators[0], (3, 2, 0, 1, 4))
    right = lax.all_gather(turned_spins.reshape(16, 2, row_count, eig_width), "gx")
    if row_count % 16:
        right = jnp.transpose(right, (1, 2, 0, 3, 4)).reshape(1, 16, 2, eig_width, eig_width)
    site_ids = lax.axis_index("gx") * sites_here + jnp.arange(sites_here, dtype=jnp.int32)
    cosine, sine_row = phase_factors(momenta, site_ids)
    fields = vectors.reshape(sites_here, 6 * eig_width)
    turned = turn_fields(fields)
    pieces = []
    group = 3
    for first in range(0, NMOM, group):
        partial = phase_partials(
            fields, turned, cosine[first : first + group], sine_row[first : first + group]
        )
        pieces.append(combine_rows(partial, row_count))
    src = source_products(local.reshape(2, row_count * 16, eig_width), source_blocks)
    left_weights, right_weights = spin_weights(op_momentum, op_gamma)
    phase_rows = jnp.concatenate(pieces, 0).astype(jnp.bfloat16)
    phase_real = phase_rows[:, :, :eig_width]
    phase_imag = phase_rows[:, :, eig_width:]
    left = jnp.concatenate(
        [
            jnp.concatenate([phase_real, -phase_imag], 2),
            jnp.concatenate([phase_imag, phase_real], 2),
            jnp.zeros((PAD - 2 * NMOM, row_count, 2 * eig_width), jnp.bfloat16),
        ],
        0,
    )
    left = jnp.transpose(left, (1, 0, 2)).reshape(row_count * PAD, 2 * eig_width)
    sink = sink_products(left, right)
    src = src.reshape(2 * NMOM, row_count, 16, eig_width)
    part = correlate(sink, src, left_weights, right_weights)
    corr, projected = finish(part, ref_vectors)
    return (corr[None], projected[None])


def solution(mesh):
    placed = (
        P("ta", "gx", None, None, None),
        P("ta", None, "gx", None, None, None),
        P(),
        P(),
        P(),
        P(),
        P(),
    )
    return jax.shard_map(
        body,
        mesh=mesh,
        in_specs=placed,
        out_specs=(P("ta", None, None, None), P("ta", None, None, None)),
        check_vma=False,
    )
```

```python
import functools
import math

import jax
import jax.numpy as jnp
import numpy as np
from jax import lax
from jax.experimental import pallas as pl
from jax.experimental.pallas import tpu as pltpu
from jax.sharding import PartitionSpec as P

EXTENT = 96
NMOM = 9


full_precision = lax.Precision.HIGHEST


def gamma_tables():
    zero_block = np.zeros((4, 4), np.float32)
    first_imag = np.array([[0, 0, 0, 1], [0, 0, 1, 0], [0, -1, 0, 0], [-1, 0, 0, 0]], np.float32)
    second_real = np.array([[0, 0, 0, -1], [0, 0, 1, 0], [0, 1, 0, 0], [-1, 0, 0, 0]], np.float32)
    third_imag = np.array([[0, 0, 1, 0], [0, 0, 0, -1], [-1, 0, 0, 0], [0, 1, 0, 0]], np.float32)
    fourth_real = np.array([[0, 0, 1, 0], [0, 0, 0, 1], [1, 0, 0, 0], [0, 1, 0, 0]], np.float32)
    gamma_list = [
        (zero_block, first_imag),
        (second_real, zero_block),
        (zero_block, third_imag),
        (fourth_real, zero_block),
    ]
    real_parts = []
    imag_parts = []
    for subset in range(16):
        prod_real = np.eye(4, dtype=np.float32)
        prod_imag = np.zeros((4, 4), np.float32)
        for position in range(4):
            if subset >> position & 1:
                factor_real, factor_imag = gamma_list[position]
                prod_real, prod_imag = (
                    prod_real @ factor_real - prod_imag @ factor_imag,
                    prod_real @ factor_imag + prod_imag @ factor_real,
                )
        real_parts.append(prod_real)
        imag_parts.append(prod_imag)
    return (np.stack(real_parts).astype(np.float32), np.stack(imag_parts).astype(np.float32))


def phase_factors(momenta, site_ids):
    xcoord = site_ids % EXTENT
    ycoord = site_ids // EXTENT % EXTENT
    zcoord = site_ids // (EXTENT * EXTENT)
    turns = jnp.pad(momenta, ((0, 128 - momenta.shape[0]), (0, 0)))
    winding = (
        turns[None, :, 0] * xcoord[:, None]
        + turns[None, :, 1] * ycoord[:, None]
        + turns[None, :, 2] * zcoord[:, None]
    ) % EXTENT
    phase_angle = winding.astype(jnp.float32) * (-2.0 * math.pi / EXTENT)
    return (jnp.cos(phase_angle), jnp.sin(phase_angle))


PAD = 24
SHARES = 4
MESH = pl.DeviceIdType.MESH


def nn_dot(left, right, precision=None):
    return lax.dot_general(
        left, right, (((1,), (0,)), ((), ())), precision=precision, preferred_element_type=jnp.float32
    )


def nt_dot(left, right):
    return lax.dot_general(
        left, right, (((1,), (1,)), ((), ())), preferred_element_type=jnp.float32
    )


def turn_kernel(fields_ref, turned_ref):
    turned_ref[...] = fields_ref[...].astype(jnp.float32).T.astype(jnp.bfloat16)


def turn_fields(fields):
    sites, wide = fields.shape
    width = wide // 6
    return pl.pallas_call(
        turn_kernel,
        grid=(6,),
        out_shape=jax.ShapeDtypeStruct((width, 6 * sites), jnp.bfloat16),
        in_specs=[pl.BlockSpec((sites, width), lambda i: (0, i))],
        out_specs=pl.BlockSpec((width, sites), lambda i: (0, i)),
        cost_estimate=pl.CostEstimate(flops=10**9, bytes_accessed=4 * sites * wide, transcendentals=0),
    )(fields)


def phase_kernel(
    chips, fields_ref, turned_ref, cos_ref, sin_ref, rows_ref, blocks_ref, mine_ref,
    out_ref, right_ref, src_ref,
    keep, give, got, leaving, coming, stage, pair_send, pair_recv, line_send, line_recv,
    hop_send, hop_recv, swap_send, swap_recv, own_send, own_recv, own_sem, stage_sem,
):
    me = lax.axis_index("gx")
    core = lax.rem(me, 2)
    chip = me // 2
    count, rows, _ = out_ref.shape
    sites, wide = fields_ref.shape
    width = wide // 6
    ways = (1, -1)
    places = (chip, chips - 1 - chip)

    barrier = pltpu.get_barrier_semaphore()
    pl.semaphore_signal(
        barrier, inc=1, device_id={"gx": me + 1 - 2 * core}, device_id_type=MESH
    )
    for way in ways:
        peer = lax.rem(me + 2 * way + 2 * chips, 2 * chips)
        pl.semaphore_signal(barrier, inc=1, device_id={"gx": peer}, device_id_type=MESH)
    pl.semaphore_wait(barrier, 3)

    def pair_copy(index):
        return pltpu.make_async_remote_copy(
            src_ref=give.at[index],
            dst_ref=got.at[index],
            send_sem=pair_send.at[index],
            recv_sem=pair_recv.at[index],
            device_id={"gx": me + 1 - 2 * core},
            device_id_type=MESH,
        )

    def line_copy(lane, index, step):
        return pltpu.make_async_remote_copy(
            src_ref=leaving.at[lane, index, step - 1],
            dst_ref=coming.at[lane, index, step - 1],
            send_sem=line_send.at[lane, index, step - 1],
            recv_sem=line_recv.at[lane, index, step - 1],
            device_id={"gx": me + 2 * ways[lane]},
            device_id_type=MESH,
        )

    partner = {"gx": me + 1 - 2 * core}

    def owner(lane, hop):
        return 2 * (chip - ways[lane] * hop) + core

    share = mine_ref.shape[0] // SHARES

    def hop_copy(lane, hop, part):
        spot = owner(lane, hop - 1)
        span = pl.ds(part * share, share)
        return pltpu.make_async_remote_copy(
            src_ref=mine_ref.at[span] if hop == 1 else right_ref.at[spot, span],
            dst_ref=right_ref.at[spot, span],
            send_sem=hop_send.at[lane, hop - 1, part],
            recv_sem=hop_recv.at[lane, hop - 1, part],
            device_id={"gx": me + 2 * ways[lane]},
            device_id_type=MESH,
        )

    def swap_copy(lane, hop, part):
        spot = owner(lane, hop)
        span = pl.ds(part * share, share)
        return pltpu.make_async_remote_copy(
            src_ref=right_ref.at[spot, span],
            dst_ref=right_ref.at[spot, span],
            send_sem=swap_send.at[lane, hop - 1, part],
            recv_sem=swap_recv.at[lane, hop - 1, part],
            device_id=partner,
            device_id_type=MESH,
        )

    own_swap = pltpu.make_async_remote_copy(
        src_ref=mine_ref,
        dst_ref=right_ref.at[me],
        send_sem=own_send,
        recv_sem=own_recv,
        device_id=partner,
        device_id_type=MESH,
    )
    own_copy = pltpu.make_async_copy(mine_ref, right_ref.at[me], own_sem)

    def pass_on(hop, part):
        for lane, place in enumerate(places):
            if hop > 0:

                @pl.when(place >= hop)
                def _():
                    hop_copy(lane, hop, part).wait_recv()
                    swap_copy(lane, hop, part).start()

            if hop + 1 < chips:

                @pl.when((place >= hop) & (place < chips - 1))
                def _():
                    hop_copy(lane, hop + 1, part).start()

    own_swap.start()
    own_copy.start()

    def stage_copy(index):
        slot = lax.rem(index, 2)
        return pltpu.make_async_copy(stage.at[slot], src_ref.at[index], stage_sem.at[slot])

    def source(index):
        shape = stage.shape[2:]
        rows_here = jnp.concatenate([rows_ref[0], rows_ref[1]], 1)
        real = blocks_ref[index, 0]
        imag = blocks_ref[index, 1]
        weights = jnp.concatenate(
            [jnp.concatenate([real, imag], 1), jnp.concatenate([imag, -real], 1)], 0
        )
        product = nt_dot(rows_here, weights).astype(jnp.bfloat16)

        @pl.when(index >= 2)
        def _():
            stage_copy(index - 2).wait()

        slot = lax.rem(index, 2)
        stage[slot, 0] = product[:, :width].reshape(shape)
        stage[slot, 1] = product[:, width:].reshape(shape)

    def phase(index):
        chosen = lax.broadcasted_iota(jnp.int32, cos_ref.shape, 1) == index
        cosine = jnp.sum(jnp.where(chosen, cos_ref[...], 0.0), 1, keepdims=True)
        sine_row = jnp.sum(jnp.where(chosen, sin_ref[...], 0.0), 1, keepdims=True)
        total = None
        for colour in range(3):
            start = 2 * colour * width
            vec_real = fields_ref[:, start : start + width].astype(jnp.float32)
            vec_imag = fields_ref[:, start + width : start + 2 * width].astype(jnp.float32)
            twist_real = (cosine * vec_real - sine_row * vec_imag).astype(jnp.bfloat16)
            twist_imag = (cosine * vec_imag + sine_row * vec_real).astype(jnp.bfloat16)
            upper = jnp.concatenate([twist_real, twist_imag], 1)
            lower = jnp.concatenate([twist_imag, -twist_real], 1)
            right = jnp.concatenate([upper, lower], 0)
            part = nn_dot(turned_ref[:, 2 * colour * sites : 2 * (colour + 1) * sites], right)
            total = part if total is None else total + part
        for spot in range(chips):
            even = total[2 * spot * rows : (2 * spot + 1) * rows]
            odd = total[(2 * spot + 1) * rows : (2 * spot + 2) * rows]
            keep[index, spot] = jnp.where(core == 0, even, odd)
            give[index, spot] = jnp.where(core == 0, odd, even).astype(jnp.bfloat16)

    def line_step(index, step):
        for lane, (way, place) in enumerate(zip(ways, places)):

            def send(block, lane=lane):
                leaving[lane, index, step - 1] = block.astype(jnp.bfloat16)
                line_copy(lane, index, step).start()

            if step < chips:
                spot = chip + way * (chips - step)

                @pl.when(place == 0)
                def _():
                    send(keep[index, spot])

                if step > 1:

                    @pl.when((place > 0) & (place < step))
                    def _():
                        line_copy(lane, index, step - 1).wait_recv()
                        send(keep[index, spot] + coming[lane, index, step - 2].astype(jnp.float32))

    def last(index):
        for lane, place in enumerate(places):

            @pl.when(place > 0)
            def _():
                line_copy(lane, index, chips - 1).wait_recv()
                keep[index, chip] = keep[index, chip] + coming[lane, index, chips - 2].astype(
                    jnp.float32
                )

            for step in range(1, chips):

                @pl.when(place < step)
                def _():
                    line_copy(lane, index, step).wait_send()

        out_ref[index] = keep[index, chip].astype(jnp.bfloat16)

    passes = [(hop, part) for hop in range(chips) for part in range(SHARES)]

    @pl.loop(0, count + chips)
    def _(turn):
        for step in range(chips, 0, -1):
            index = turn - step

            @pl.when((index >= 0) & (index < count))
            def _():
                if step == 1:
                    pair_copy(index).wait()
                    keep[index] = keep[index] + got[index].astype(jnp.float32)
                if step < chips:
                    line_step(index, step)
                else:
                    last(index)

        for place, (hop, part) in enumerate(passes[: count + chips]):

            @pl.when(turn == place)
            def _():
                pass_on(hop, part)

        @pl.when(turn < count)
        def _():
            phase(turn)
            pair_copy(turn).start()
            source(turn)
            stage_copy(turn).start()

    for hop, part in passes[count + chips :]:
        pass_on(hop, part)
    for lane, place in enumerate(places):
        for hop in range(1, chips):
            for part in range(SHARES):

                @pl.when(place >= hop)
                def _():
                    swap_copy(lane, hop, part).wait()

                @pl.when((place >= hop - 1) & (place < chips - 1))
                def _():
                    hop_copy(lane, hop, part).wait_send()

    own_swap.wait()
    own_copy.wait()
    for index in range(max(count - 2, 0), count):
        stage_copy(index).wait()


def phase_rows_of(fields, turned, cosine, sine_row, rows, source_blocks, mine):
    sites, wide = fields.shape
    width = wide // 6
    count = source_blocks.shape[0]
    size = lax.axis_size("gx")
    chips = size // 2
    row_count = mine.shape[2]
    vmem = pl.BlockSpec(memory_space=pltpu.VMEM)
    hbm = pl.BlockSpec(memory_space=pl.ANY)
    blocks = (count, chips, row_count, 2 * width)
    moves = (2, count, chips - 1, row_count, 2 * width)
    product = (2, row_count, 16, width)
    return pl.pallas_call(
        functools.partial(phase_kernel, chips),
        out_shape=(
            jax.ShapeDtypeStruct((count, row_count, 2 * width), jnp.bfloat16),
            jax.ShapeDtypeStruct((size, *mine.shape), jnp.bfloat16),
            jax.ShapeDtypeStruct((count, *product), jnp.bfloat16),
        ),
        in_specs=[vmem] * 7,
        out_specs=(vmem, hbm, hbm),
        scratch_shapes=[
            pltpu.VMEM(blocks, jnp.float32),
            pltpu.VMEM(blocks, jnp.bfloat16),
            pltpu.VMEM(blocks, jnp.bfloat16),
            pltpu.VMEM(moves, jnp.bfloat16),
            pltpu.VMEM(moves, jnp.bfloat16),
            pltpu.VMEM((2, *product), jnp.bfloat16),
            pltpu.SemaphoreType.DMA((count,)),
            pltpu.SemaphoreType.DMA((count,)),
            pltpu.SemaphoreType.DMA((2, count, chips - 1)),
            pltpu.SemaphoreType.DMA((2, count, chips - 1)),
            pltpu.SemaphoreType.DMA((2, chips - 1, SHARES)),
            pltpu.SemaphoreType.DMA((2, chips - 1, SHARES)),
            pltpu.SemaphoreType.DMA((2, chips - 1, SHARES)),
            pltpu.SemaphoreType.DMA((2, chips - 1, SHARES)),
            pltpu.SemaphoreType.DMA,
            pltpu.SemaphoreType.DMA,
            pltpu.SemaphoreType.DMA,
            pltpu.SemaphoreType.DMA((2,)),
        ],
        compiler_params=pltpu.CompilerParams(
            collective_id=1, has_side_effects=True, vmem_limit_bytes=58 * 2**20
        ),
        cost_estimate=pl.CostEstimate(
            flops=32 * count * sites * width * width,
            bytes_accessed=4 * sites * wide,
            transcendentals=0,
        ),
    )(fields, turned, cosine, sine_row, rows, source_blocks, mine)


def sink_kernel(left_ref, right_ref, out_ref):
    width = right_ref.shape[-1]
    shape = out_ref.shape[1:]
    right = jnp.concatenate(
        [
            jnp.concatenate(
                [right_ref[:, spin, part].reshape(-1, width) for part in range(2)], 0
            )
            for spin in range(2)
        ],
        1,
    )
    product = nn_dot(left_ref[...], right).astype(jnp.bfloat16)
    out_ref[0] = product[:, :width].reshape(shape)
    out_ref[1] = product[:, width:].reshape(shape)


def sink_products(left, right):
    high = left.shape[0]
    owners, spins, _, depth, width = right.shape
    return pl.pallas_call(
        sink_kernel,
        grid=(spins // 2,),
        out_shape=jax.ShapeDtypeStruct((spins, high // PAD, PAD, width), jnp.bfloat16),
        in_specs=[
            pl.BlockSpec((high, 2 * width), lambda x: (0, 0)),
            pl.BlockSpec((owners, 2, 2, depth, width), lambda x: (0, x, 0, 0, 0)),
        ],
        out_specs=pl.BlockSpec((2, high // PAD, PAD, width), lambda x: (x, 0, 0, 0)),
        cost_estimate=pl.CostEstimate(
            flops=4 * spins * high * width * width,
            bytes_accessed=4 * spins * high * width,
            transcendentals=0,
        ),
    )(left, right)


def three_parts(value):
    parts = []
    for _ in range(3):
        part = value.astype(jnp.bfloat16)
        parts.append(part)
        value = value - part.astype(jnp.float32)
    return parts


def correlate_kernel(sink_ref, src_ref, left_ref, right_ref, out_ref, total_ref):
    step = pl.program_id(0)
    width = sink_ref.shape[-1]
    picks = sink_ref.shape[1]
    product = None
    for start in range(0, picks, 2):
        pair = range(start, start + 2)
        first = jnp.concatenate([src_ref[:, :, index].reshape(-1, width) for index in pair], 1)
        second = jnp.concatenate([sink_ref[:, index].reshape(-1, width) for index in pair], 1)
        part = nt_dot(first, second)
        product = part if product is None else product + part

    @pl.when(step == 0)
    def _():
        total_ref[...] = product

    @pl.when(step > 0)
    def _():
        total_ref[...] += product

    @pl.when(step == pl.num_programs(0) - 1)
    def _():
        high, wide = total_ref.shape
        ops = left_ref.shape[1] // 4
        span = wide // 4
        row_spin = lax.broadcasted_iota(jnp.int32, (high, 1), 0) // 4 % 4
        answer = jnp.zeros((ops, ops), jnp.float32)
        for spin in range(4):
            spread = jnp.zeros((high, 4 * ops), jnp.float32)
            for part in three_parts(total_ref[:, spin * span : (spin + 1) * span]):
                spread = spread + nn_dot(part, left_ref[...])
            lifted = spread[:, :ops]
            for other in range(1, 4):
                lifted = jnp.where(
                    row_spin == other, spread[:, other * ops : (other + 1) * ops], lifted
                )
            for part in three_parts(lifted):
                answer = answer + nn_dot(right_ref[spin], part)
        half = ops // 2
        answer = answer.T
        real = answer[:half] - pltpu.roll(answer[half:], half, 1)
        imag = pltpu.roll(answer[:half], half, 1) + answer[half:]
        lane = lax.broadcasted_iota(jnp.int32, real.shape, 1)
        out_ref[...] = jnp.where(lane < half, real, pltpu.roll(imag, half, 1))


def correlate(sink, src, left, right):
    spins, rows, pad, width = sink.shape
    count = 2 * src.shape[0]
    picks = 4
    ops = left.shape[1] // 4
    return pl.pallas_call(
        correlate_kernel,
        grid=(rows // picks,),
        out_shape=jax.ShapeDtypeStruct((ops // 2, ops), jnp.float32),
        in_specs=[
            pl.BlockSpec((spins, picks, pad, width), lambda r: (0, r, 0, 0)),
            pl.BlockSpec((count // 2, 2, picks, spins, width), lambda r: (0, 0, r, 0, 0)),
            pl.BlockSpec(left.shape, lambda r: (0, 0)),
            pl.BlockSpec(right.shape, lambda r: (0, 0, 0)),
        ],
        out_specs=pl.BlockSpec((ops // 2, ops), lambda r: (0, 0)),
        scratch_shapes=[pltpu.VMEM((count * spins, spins * pad), jnp.float32)],
        cost_estimate=pl.CostEstimate(
            flops=2 * rows * spins * pad * count * spins * width,
            bytes_accessed=2 * rows * spins * width * (pad + count),
            transcendentals=0,
        ),
    )(sink, src, left, right)


def finish_kernel(
    groups, slices, part_ref, basis_ref, turned_ref, corr_ref, proj_ref,
    slots, squares, send_sem, recv_sem, square_send, square_recv,
):
    me = lax.axis_index("gx")
    here = lax.axis_index("ta")
    barrier = pltpu.get_barrier_semaphore()
    for step in range(1, groups):
        peer = lax.rem(me + step, groups)
        pl.semaphore_signal(barrier, inc=1, device_id={"gx": peer}, device_id_type=MESH)
    for step in range(1, slices):
        peer = lax.rem(here + step, slices)
        pl.semaphore_signal(barrier, inc=1, device_id={"ta": peer}, device_id_type=MESH)
    pl.semaphore_wait(barrier, groups + slices - 2)
    copies = []
    for step in range(1, groups):
        copies.append(
            pltpu.make_async_remote_copy(
                src_ref=part_ref,
                dst_ref=slots.at[me],
                send_sem=send_sem.at[step],
                recv_sem=recv_sem.at[step],
                device_id={"gx": lax.rem(me + step, groups)},
                device_id_type=MESH,
            )
        )
    for copy in copies:
        copy.start()
    slots[me] = part_ref[...]
    for copy in copies:
        copy.wait()
    total = slots[0]
    for index in range(1, groups):
        total = total + slots[index]
    half = total.shape[0]
    real = total[:, :half]
    imag = total[:, half:]
    corr_ref[0] = real
    corr_ref[1] = imag

    def product(left, right):
        return nn_dot(left, right, full_precision)

    mid_real = product(real, basis_ref[0]) - product(imag, basis_ref[1])
    mid_imag = product(real, basis_ref[1]) + product(imag, basis_ref[0])
    raw_real = product(turned_ref[0], mid_real) + product(turned_ref[1], mid_imag)
    raw_imag = product(turned_ref[0], mid_imag) - product(turned_ref[1], mid_real)
    vectors = raw_real.shape[0]
    square = jnp.sum(
        jnp.sum(raw_real * raw_real + raw_imag * raw_imag, 1, keepdims=True), 0, keepdims=True
    ) / (2 * vectors * vectors)
    squares[here] = jnp.broadcast_to(square, squares.shape[1:])
    copies = []
    for step in range(1, slices):
        copies.append(
            pltpu.make_async_remote_copy(
                src_ref=squares.at[here],
                dst_ref=squares.at[here],
                send_sem=square_send.at[step],
                recv_sem=square_recv.at[step],
                device_id={"ta": lax.rem(here + step, slices)},
                device_id_type=MESH,
            )
        )
    for copy in copies:
        copy.start()
    for copy in copies:
        copy.wait()
    scale = lax.rsqrt(squares[0] + 1e-06)[:vectors]
    proj_ref[0] = (raw_real * scale)[:, :vectors]
    proj_ref[1] = (raw_imag * scale)[:, :vectors]


def finish(part, ref_vectors):
    groups = lax.axis_size("gx")
    slices = lax.axis_size("ta")
    half, wide = part.shape
    vectors = ref_vectors.shape[-1]
    basis = jnp.pad(ref_vectors, ((0, 0), (0, 0), (0, 128 - vectors)))
    turned = jnp.transpose(ref_vectors, (0, 2, 1))
    vmem = pl.BlockSpec(memory_space=pltpu.VMEM)
    return pl.pallas_call(
        functools.partial(finish_kernel, groups, slices),
        out_shape=(
            jax.ShapeDtypeStruct((2, half, half), jnp.float32),
            jax.ShapeDtypeStruct((2, vectors, vectors), jnp.float32),
        ),
        in_specs=[vmem, vmem, vmem],
        out_specs=(vmem, vmem),
        scratch_shapes=[
            pltpu.VMEM((groups, half, wide), jnp.float32),
            pltpu.VMEM((slices, 8, 128), jnp.float32),
            pltpu.SemaphoreType.DMA((groups,)),
            pltpu.SemaphoreType.DMA((groups,)),
            pltpu.SemaphoreType.DMA((slices,)),
            pltpu.SemaphoreType.DMA((slices,)),
        ],
        compiler_params=pltpu.CompilerParams(collective_id=0, has_side_effects=True),
    )(part, basis, turned)


def spin_weights(op_momentum, op_gamma):
    table_real, table_imag = gamma_tables()
    chosen = (op_gamma[:, None] == jnp.arange(16, dtype=jnp.int32)[None, :]).astype(jnp.float32)
    gre = jnp.einsum("ig,gax->iax", chosen, jnp.asarray(table_real), precision=full_precision)
    gim = jnp.einsum("ig,gax->iax", chosen, jnp.asarray(table_imag), precision=full_precision)
    moment = (op_momentum[:, None] == jnp.arange(NMOM, dtype=jnp.int32)[None, :]).astype(
        jnp.float32
    )
    chiral = jnp.asarray(np.array([1.0, 1.0, -1.0, -1.0], np.float32))
    ops = op_gamma.shape[0]
    gre = gre * chiral[None, :, None]
    gim = gim * chiral[None, :, None]
    left = jnp.stack([jnp.stack([gre, gim], 0), jnp.stack([-gim, gre], 0)], 0)
    left = jnp.transpose(left, (4, 0, 3, 1, 2))[:, :, None] * jnp.transpose(moment)[
        None, None, :, None, None, :
    ]
    left = left.reshape(4, 2 * NMOM, 8 * ops)
    left = jnp.pad(left, ((0, 0), (0, PAD - 2 * NMOM), (0, 0))).reshape(4 * PAD, 8 * ops)
    right = jnp.stack([jnp.stack([gre, -gim], 0), jnp.stack([gim, gre], 0)], 0)
    right = jnp.transpose(right, (4, 1, 2, 0, 3))[:, :, :, None, :, None, :] * moment[
        None, None, :, :, None, None, None
    ]
    right = jnp.broadcast_to(right, (4, 2, ops, NMOM, 2, 4, 4)).reshape(4, 2 * ops, 32 * NMOM)
    return left.astype(jnp.bfloat16), right.astype(jnp.bfloat16)


def body(eigvecs, perambulators, source_blocks, momenta, op_momentum, op_gamma, ref_vectors):
    vectors = eigvecs[0]
    sites_here = vectors.shape[0]
    eig_width = vectors.shape[-1]
    size = lax.axis_size("gx")
    row_count = eig_width // size
    local = perambulators[0].reshape(2, row_count, 16, eig_width)
    turned_spins = jnp.transpose(perambulators[0], (3, 2, 0, 1, 4))
    mine = turned_spins.reshape(16, 2, row_count, eig_width)
    site_ids = lax.axis_index("gx") * sites_here + jnp.arange(sites_here, dtype=jnp.int32)
    cosine, sine_row = phase_factors(momenta, site_ids)
    fields = vectors.reshape(sites_here, 6 * eig_width)
    turned = turn_fields(fields)
    left_weights, right_weights = spin_weights(op_momentum, op_gamma)
    rows = local.reshape(2, row_count * 16, eig_width)
    phase_rows, right, src = phase_rows_of(
        fields, turned, cosine, sine_row, rows, source_blocks, mine
    )
    if row_count % 16:
        right = jnp.transpose(right, (1, 2, 0, 3, 4)).reshape(1, 16, 2, eig_width, eig_width)
    phase_real = phase_rows[:, :, :eig_width]
    phase_imag = phase_rows[:, :, eig_width:]
    left = jnp.concatenate(
        [
            jnp.concatenate([phase_real, -phase_imag], 2),
            jnp.concatenate([phase_imag, phase_real], 2),
            jnp.zeros((PAD - 2 * NMOM, row_count, 2 * eig_width), jnp.bfloat16),
        ],
        0,
    )
    left = jnp.transpose(left, (1, 0, 2)).reshape(row_count * PAD, 2 * eig_width)
    sink = sink_products(left, right)
    part = correlate(sink, src, left_weights, right_weights)
    corr, projected = finish(part, ref_vectors)
    return (corr[None], projected[None])


def solution(mesh):
    placed = (
        P("ta", "gx", None, None, None),
        P("ta", None, "gx", None, None, None),
        P(),
        P(),
        P(),
        P(),
        P(),
    )
    return jax.shard_map(
        body,
        mesh=mesh,
        in_specs=placed,
        out_specs=(P("ta", None, None, None), P("ta", None, None, None)),
        check_vma=False,
    )
```
